256 devices in a mesh: seq: 16 (over z, core), heads: 4 (over x), batch: 4 (over y).
Axes of the slice: x: 4, y: 4, z: 8, core: 2. Of those that a mesh axis runs over, the one named last changes fastest.
Arguments:
- queries: bfloat16 [4, 4096, 8192], P('batch', 'seq', 'heads'), may hold values from -160 to 160
- keys: bfloat16 [4, 4096, 1024], P('batch', 'seq', 'heads'), may hold values from -7 to 7
- values: bfloat16 [4, 4096, 1024], P('batch', 'seq', 'heads'), may hold values from -6 to 6
- doc_lengths: int32 [4, 16], P('batch'), may hold values from 1 to 2176, 4096 in all within a row
- out_weight: bfloat16 [8192, 8192], P('heads', 'batch'), may hold values from -0.0625 to 0.0625
Outputs:
- projected: bfloat16 [4, 4096, 8192], P('heads', 'seq', 'batch')
The draws below stay inside these ranges and needn't reach their ends.
Inputs may be any that keep to these rules, and one draw needn't show every extreme that they name: `doc_lengths`: each row sums to 4096; no document is longer than 2176 tokens and one is exactly 2176.
All inputs are finite; a program needn't handle non-finite values.
Results may differ from the reference program's by a relative error of at most 0.012.
Values may be sent and summed in bfloat16 or wider, within the bound.
A program may use at most 64 MiB of HBM per device.

```python
import math
import jax
import jax.numpy as jnp
import numpy as np
from jax import lax

QUERY_HEAD_COUNT = 64
VALUE_KEY_HEADS = 8
HEAD_WIDTH = 128
D = 8192
DOCS = 16
QBLOCK = 128
PACKED_BATCH = 4
PACKED_LENGTH = 4096
LONGEST = 2176


def shared_keys(key):
    sampled_values = jax.random.normal(jax.random.fold_in(key, 11), (PACKED_BATCH, PACKED_LENGTH, VALUE_KEY_HEADS, HEAD_WIDTH), jnp.float32)
    sampled_values = jnp.clip(sampled_values, -6.0, 6.0)
    return sampled_values


def draw_keys(key, part):
    sampled_values = shared_keys(key)
    return sampled_values.reshape(PACKED_BATCH, PACKED_LENGTH, VALUE_KEY_HEADS * HEAD_WIDTH).astype(jnp.bfloat16)


def draw_queries(key, part):
    sampled_values = jax.random.normal(jax.random.fold_in(key, 21), (PACKED_BATCH, PACKED_LENGTH, QUERY_HEAD_COUNT, HEAD_WIDTH), jnp.float32)
    sampled_values = jnp.clip(sampled_values, -6.0, 6.0)
    return sampled_values.reshape(PACKED_BATCH, PACKED_LENGTH, QUERY_HEAD_COUNT * HEAD_WIDTH).astype(jnp.bfloat16)


def level_of(stream_key, dims, shards, low, top_value):
    def one(dim, blocks):
        draws = jax.random.uniform(jax.random.fold_in(jax.random.fold_in(stream_key, 6), dim), (blocks,), jnp.float32, low / len(shards), top_value / len(shards))
        return jnp.repeat(jnp.exp(draws), dims[dim] // blocks).reshape((-1,) + (1,) * (len(dims) - dim - 1))

    loudness = one(*shards[0])
    for cut in shards[1:]:
        loudness = loudness * one(*cut)
    return loudness


def length_profile(count, total, limit, lean):
    portions = [(1 << 20) // math.isqrt(grade ** lean) + 1 for grade in range(2, count + 1)]
    rest, given = total - limit - (count - 1), [1] * (count - 1)
    while rest > 0:
        candidates = [i for i in range(count - 1) if given[i] < limit]
        whole, budget = sum([portions[i] for i in candidates]), rest
        for i in candidates:
            more = min(limit - given[i], max(1, budget * portions[i] // whole), rest)
            given[i] = given[i] + more
            rest = rest - more
    return np.array([limit] + given)


def ragged_sizes(key, count, total, bound, skew):
    if count == 2:
        one = jax.random.randint(key, (), max(1, total - bound), min(bound, total - 1) + 1)
        return jnp.stack([one, total - one])
    tallies = jnp.asarray(length_profile(count, total, bound, skew), jnp.int32)
    twos = (count - 1) // 2
    giver, receiver = tallies[1:1 + 2 * twos:2], tallies[2:2 + 2 * twos:2]
    margin = jnp.minimum(giver - 1, bound - receiver)
    shifted = jax.random.randint(jax.random.fold_in(key, 1), (twos,), 0, 1 << 20) % (margin + 1)
    tallies = tallies.at[1:1 + 2 * twos:2].set(giver - shifted).at[2:2 + 2 * twos:2].set(receiver + shifted)
    return tallies[jax.random.permutation(jax.random.fold_in(key, 2), count)]


def centred(own_key, dims, width, limit, pieces=(), held_as=jnp.bfloat16):
    entries = jax.random.normal(own_key, dims, jnp.float32) * width
    if len(pieces) > 0:
        entries = level_of(own_key, dims, pieces, -0.22, 0.18) * entries
    return jnp.clip(entries, min=-limit, max=limit).astype(held_as)


def setup_inputs(seed: int = 0) -> dict:
    arg_keys = jax.random.split(jax.random.key(seed), 6)
    queries = draw_queries(jax.random.fold_in(arg_keys[5], 71), 0)
    keys = draw_keys(jax.random.fold_in(arg_keys[5], 71), 0)
    values = centred(arg_keys[2], (PACKED_BATCH, PACKED_LENGTH, VALUE_KEY_HEADS * HEAD_WIDTH), 1.0, 6.0, ((0, 4), (1, 16), (2, 4)))
    doc_lengths = jax.vmap(lambda own: ragged_sizes(own, DOCS, PACKED_LENGTH, LONGEST, 2))(jax.random.split(arg_keys[3], PACKED_BATCH)).reshape((PACKED_BATCH, DOCS)).astype(jnp.int32)
    out_weight = centred(arg_keys[4], (QUERY_HEAD_COUNT * HEAD_WIDTH, D), (QUERY_HEAD_COUNT * HEAD_WIDTH) ** -0.5, 0.0625, ((0, 4), (1, 4)))
    return dict(queries=queries, keys=keys, values=values, doc_lengths=doc_lengths, out_weight=out_weight)


def document_of(lengths):
    doc_ends = jnp.cumsum(lengths)
    positions = jnp.arange(PACKED_LENGTH, dtype=jnp.int32)
    return jnp.sum((positions[:, None] >= doc_ends[None, :]).astype(jnp.int32), axis=1)


def attend_sequence(bundle):
    query_sequence, key_sequence, value_sequence, lengths = bundle
    group_width = QUERY_HEAD_COUNT // VALUE_KEY_HEADS
    key_span = min(LONGEST + QBLOCK, PACKED_LENGTH)
    doc_ids = document_of(lengths)
    query_head_rows = query_sequence.reshape(PACKED_LENGTH, VALUE_KEY_HEADS, group_width, HEAD_WIDTH)
    key_head_rows = key_sequence.reshape(PACKED_LENGTH, VALUE_KEY_HEADS, HEAD_WIDTH)
    value_head_rows = value_sequence.reshape(PACKED_LENGTH, VALUE_KEY_HEADS, HEAD_WIDTH)

    def one_block(block_index):
        q_start = (block_index * QBLOCK).astype(jnp.int32)
        k_start = jnp.clip(q_start + QBLOCK - key_span, 0, PACKED_LENGTH - key_span).astype(jnp.int32)
        q_block = lax.dynamic_slice_in_dim(query_head_rows, q_start, QBLOCK, 0).astype(jnp.float32)
        k_block = lax.dynamic_slice_in_dim(key_head_rows, k_start, key_span, 0).astype(jnp.float32)
        v_block = lax.dynamic_slice_in_dim(value_head_rows, k_start, key_span, 0).astype(jnp.float32)
        scores = jnp.einsum("qhgd,khd->hgqk", q_block, k_block, precision=lax.Precision.HIGHEST) * (HEAD_WIDTH ** -0.5)
        q_pos = q_start + jnp.arange(QBLOCK, dtype=jnp.int32)
        k_pos = k_start + jnp.arange(key_span, dtype=jnp.int32)
        q_doc = lax.dynamic_slice_in_dim(doc_ids, q_start, QBLOCK, 0)
        k_doc = lax.dynamic_slice_in_dim(doc_ids, k_start, key_span, 0)
        allowed = (q_doc[:, None] == k_doc[None, :]) & (k_pos[None, :] <= q_pos[:, None])
        scores = jnp.where(allowed, scores, -jnp.inf)
        highest = jnp.max(scores, axis=-1, keepdims=True)
        weights = jnp.exp(scores - highest)
        denominator = jnp.sum(weights, axis=-1)
        rounded = lax.optimization_barrier(weights.astype(jnp.bfloat16)).astype(jnp.float32)
        summed = jnp.einsum("hgqk,khd->qhgd", rounded, v_block, precision=lax.Precision.HIGHEST)
        result = summed / jnp.transpose(denominator, (2, 0, 1))[..., None]
        return result.reshape(QBLOCK, QUERY_HEAD_COUNT * HEAD_WIDTH).astype(jnp.bfloat16)

    outputs = lax.map(one_block, jnp.arange(PACKED_LENGTH // QBLOCK, dtype=jnp.int32))
    return outputs.reshape(PACKED_LENGTH, QUERY_HEAD_COUNT * HEAD_WIDTH)


def reference(queries, keys, values, doc_lengths, out_weight):
    attended = lax.map(attend_sequence, (queries, keys, values, doc_lengths))
    flat_rows = attended.reshape(PACKED_BATCH * PACKED_LENGTH, QUERY_HEAD_COUNT * HEAD_WIDTH).astype(jnp.float32)
    projected = jnp.dot(flat_rows, out_weight.astype(jnp.float32), precision=lax.Precision.HIGHEST)
    return projected.astype(jnp.bfloat16).reshape(PACKED_BATCH, PACKED_LENGTH, D)
```

```python
import functools

import jax
import jax.numpy as jnp
from jax import lax
from jax.experimental import pallas as pl
from jax.experimental.pallas import tpu as pltpu
from jax.sharding import PartitionSpec as P

MESH = pl.DeviceIdType.MESH
HEAD = 128
DOCS = 16
CHUNKS = 8
LOWEST = -1e30
SCALE = (HEAD ** -0.5) * 1.4426950408889634


def kernel(
    q_hbm, k_hbm, v_hbm, docs, w_hbm, out_hbm,
    qv, qt, kv, vt, bias, first, top, total, acc, gathered, weight, partial, near, final, outv,
    load_sem, kv_recv, next_send, side_send, far_send, ag_send, ag_recv, rs_send, rs_recv, out_sem,
):
    s = lax.axis_index("seq")
    x = lax.axis_index("heads")
    y = lax.axis_index("batch")
    seqs, xs, ys = lax.axis_size("seq"), lax.axis_size("heads"), lax.axis_size("batch")
    z = s // 2
    odd = s % 2
    rows = qv.shape[0]
    heads = qt.shape[0]
    half = rows // 2
    span = rows // CHUNKS
    part = span // 2
    right, left, across = (x + 1) % xs, (x + xs - 1) % xs, (x + 2) % xs
    up, down = (y + 1) % ys, (y + ys - 1) % ys

    def remote(src, dst, send, recv, **where):
        return pltpu.make_async_remote_copy(
            src_ref=src, dst_ref=dst, send_sem=send, recv_sem=recv, device_id=where, device_id_type=MESH
        )

    load_k = pltpu.make_async_copy(k_hbm.at[0], kv.at[0, 0], load_sem.at[0])
    load_v = pltpu.make_async_copy(v_hbm.at[0], kv.at[0, 1], load_sem.at[1])
    load_q = pltpu.make_async_copy(q_hbm.at[0], qv, load_sem.at[2])
    load_w = pltpu.make_async_copy(w_hbm, weight, load_sem.at[3])
    load_k.start()
    load_v.start()
    load_q.start()
    load_w.start()

    barrier = pltpu.get_barrier_semaphore()
    for by in (1, 2, seqs - 2, seqs - 1):
        pl.semaphore_signal(barrier, inc=1, device_id={"seq": (s + by) % seqs}, device_id_type=MESH)
    for peer in (right, left):
        pl.semaphore_signal(barrier, inc=1, device_id={"heads": peer}, device_id_type=MESH)
    for peer in (up, down):
        pl.semaphore_signal(barrier, inc=1, device_id={"batch": peer}, device_id_type=MESH)
    pl.semaphore_wait(barrier, 8)

    def to_next(t, i):
        slot = jnp.minimum(2 * t + 2, 8)
        return remote(
            kv.at[2 * t, i], kv.at[slot, i], next_send.at[t, i], kv_recv.at[slot, i],
            seq=jnp.minimum(s + 2, seqs - 1),
        )

    def to_side(t, i):
        slot = jnp.maximum(2 * t + 1 - 2 * odd, 0)
        return remote(
            kv.at[2 * t, i], kv.at[slot, i], side_send.at[t, i], kv_recv.at[slot, i], seq=s + 1 - 2 * odd
        )

    def to_far(i):
        return remote(
            kv.at[8, i, half:], kv.at[9, i, half:], far_send.at[i], kv_recv.at[9, i], seq=jnp.minimum(s + 1, seqs - 1)
        )

    def sends_next(t):
        return (z >= t) & (t <= 3) & (s + 2 < seqs)

    def sends_side(t):
        return (z >= t) & (t >= odd) & (t <= 3 + odd)

    sends_far = (z >= 4) & (s + 1 < seqs)

    def forward(t, i):
        @pl.when(sends_next(t))
        def _():
            to_next(t, i).start()

        @pl.when(sends_side(t))
        def _():
            to_side(t, i).start()

        @pl.when(sends_far & (t == 4))
        def _():
            to_far(i).start()

    def arrived(slot, i):
        remote(kv.at[slot, i], kv.at[slot, i], next_send.at[0, i], kv_recv.at[slot, i], seq=s).wait_recv()

    load_k.wait()
    forward(0, 0)
    load_v.wait()
    forward(0, 1)

    q_pos = s * rows + lax.broadcasted_iota(jnp.int32, (1, rows), 1)
    starts = jnp.zeros((1, rows), jnp.int32)
    ended = jnp.int32(0)
    for d in range(DOCS):
        length = docs[0, d]
        ended = ended + length
        starts = starts + jnp.where(q_pos >= ended, length, 0)
    first[...] = starts
    top[...] = jnp.full(top.shape, LOWEST, jnp.float32)
    total[...] = jnp.zeros(total.shape, jnp.float32)

    load_q.wait()

    @pl.loop(0, heads)
    def _(h):
        qt[h] = qv[:, pl.ds(pl.multiple_of(h * HEAD, HEAD), HEAD)].T
        acc[h] = jnp.zeros((HEAD, rows), jnp.float32)

    def attend(slot, low, columns):
        count = rows - low
        for g in range(2):
            vt[g, :, :count] = kv[slot, 1, low:, g * HEAD : (g + 1) * HEAD].T
        k_pos = (s - slot) * rows + low + lax.broadcasted_iota(jnp.int32, (count, columns), 0)
        q_all = s * rows + lax.broadcasted_iota(jnp.int32, (count, columns), 1)
        seen = (k_pos >= first[:, :columns]) & (k_pos <= q_all)
        bias[:count, :columns] = jnp.where(seen, 0.0, LOWEST)

        @pl.loop(0, heads // 4)
        def _(block):
            g = block // 2
            keys = kv[slot, 0, low:, pl.ds(pl.multiple_of(g * HEAD, HEAD), HEAD)]
            values = vt[g, :, :count]
            for u in range(4):
                h = block * 4 + u
                scores = jnp.dot(keys, qt[h, :, :columns], preferred_element_type=jnp.float32)
                scores = scores + bias[:count, :columns]
                before = top[h, :, :columns]
                now = jnp.maximum(before, jnp.max(scores, axis=0, keepdims=True))
                weights = jnp.exp2((scores - now) * SCALE)
                shrink = jnp.exp2((before - now) * SCALE)
                top[h, :, :columns] = now
                total[h, :, :columns] = total[h, :, :columns] * shrink + jnp.sum(weights, axis=0, keepdims=True)
                summed = jnp.dot(values, weights.astype(jnp.bfloat16), preferred_element_type=jnp.float32)
                acc[h, :, :columns] = acc[h, :, :columns] * shrink + summed

    @pl.loop(0, 5)
    def _(t):
        @pl.when(z >= t)
        def _():
            @pl.when(t >= 1)
            def _():
                for i in range(2):
                    arrived(2 * t, i)
                    forward(t, i)

            attend(2 * t, 0, rows)

        @pl.when((z >= t) & (t + odd >= 1) & (t <= 3 + (1 - odd)))
        def _():
            slot = jnp.clip(2 * t - 1 + 2 * odd, 0, 9)
            for i in range(2):
                arrived(slot, i)
            attend(slot, 0, rows)

    @pl.when(s >= 9)
    def _():
        for i in range(2):
            remote(
                kv.at[9, i, half:], kv.at[9, i, half:], far_send.at[i], kv_recv.at[9, i], seq=s
            ).wait_recv()
        attend(9, half, half)

    @pl.loop(0, heads)
    def _(h):
        done = acc[h] * (1.0 / total[h])
        turned = done.T.astype(jnp.bfloat16)
        for c in range(CHUNKS):
            gathered[c, y, :, pl.ds(pl.multiple_of(h * HEAD, HEAD), HEAD)] = turned[c * span : (c + 1) * span]

    def own(c):
        return (
            remote(gathered.at[c, y], gathered.at[c, y], ag_send.at[c, 0], ag_recv.at[c, 0], batch=up),
            remote(gathered.at[c, y], gathered.at[c, y], ag_send.at[c, 1], ag_recv.at[c, 1], batch=down),
        )

    def from_neighbours(c):
        return (
            remote(gathered.at[c, down], gathered.at[c, down], ag_send.at[c, 0], ag_recv.at[c, 0], batch=up),
            remote(gathered.at[c, up], gathered.at[c, up], ag_send.at[c, 1], ag_recv.at[c, 1], batch=down),
        )

    def relays(c):
        a, b = gathered.at[c, down, :part], gathered.at[c, up, part:]
        return (
            remote(a, a, ag_send.at[c, 2], ag_recv.at[c, 2], batch=up),
            remote(b, b, ag_send.at[c, 3], ag_recv.at[c, 3], batch=down),
        )

    def from_far(c):
        opposite = (y + 2) % ys
        a, b = gathered.at[c, opposite, :part], gathered.at[c, opposite, part:]
        return (
            remote(a, a, ag_send.at[c, 2], ag_recv.at[c, 2], batch=up),
            remote(b, b, ag_send.at[c, 3], ag_recv.at[c, 3], batch=down),
        )

    def sums(c):
        table = (
            (partial.at[c, across, :part], near.at[c, 0], right),
            (partial.at[c, across, part:], near.at[c, 1], left),
            (partial.at[c, right, part:], final.at[c, 0, part:], right),
            (partial.at[c, left, :part], final.at[c, 1, :part], left),
            (partial.at[c, right, :part], final.at[c, 0, :part], right),
            (partial.at[c, left, part:], final.at[c, 1, part:], left),
        )
        return [
            functools.partial(remote, src, dst, rs_send.at[c, i], rs_recv.at[c, i], heads=to)
            for i, (src, dst, to) in enumerate(table)
        ]

    def start_own(c):
        for copy in own(c):
            copy.start()

    def relay(c):
        for arriving, onward in zip(from_neighbours(c), relays(c)):
            arriving.wait_recv()
            onward.start()

    wide = 512

    def project(c):
        for arriving in from_far(c):
            arriving.wait_recv()
        lhs = gathered[c].reshape(ys * span, -1)

        @pl.loop(0, weight.shape[1] // wide)
        def _(n):
            columns = pl.ds(pl.multiple_of(n * wide, wide), wide)
            product = jnp.dot(lhs, weight[:, columns], preferred_element_type=jnp.float32)
            partial[c, :, :, columns] = product.astype(jnp.bfloat16).reshape(ys, span, wide)

    def send_first(c):
        for copy in sums(c)[:4]:
            copy().start()

    def send_second(c):
        copies = sums(c)
        copies[0]().wait_recv()
        partial[c, right, :part] = (
            partial[c, right, :part].astype(jnp.float32) + near[c, 0].astype(jnp.float32)
        ).astype(jnp.bfloat16)
        copies[4]().start()
        copies[1]().wait_recv()
        partial[c, left, part:] = (
            partial[c, left, part:].astype(jnp.float32) + near[c, 1].astype(jnp.float32)
        ).astype(jnp.bfloat16)
        copies[5]().start()

    def write(c):
        return pltpu.make_async_copy(
            outv.at[pl.ds(pl.multiple_of(c * span, span), span)],
            out_hbm.at[0, pl.ds(pl.multiple_of(c * span, span), span)],
            out_sem.at[c],
        )

    def finish(c):
        copies = sums(c)
        for i in range(2, 6):
            copies[i]().wait_recv()
        value = (
            partial[c, x].astype(jnp.float32)
            + final[c, 0].astype(jnp.float32)
            + final[c, 1].astype(jnp.float32)
        )
        outv[pl.ds(pl.multiple_of(c * span, span), span)] = value.astype(jnp.bfloat16)
        write(c).start()

    start_own(0)
    start_own(1)
    load_w.wait()

    @pl.loop(0, CHUNKS + 3)
    def _(i):
        def chunk(by):
            return jnp.clip(i + by, 0, CHUNKS - 1)

        @pl.when(i < CHUNKS)
        def _():
            relay(chunk(0))

        @pl.when(i + 2 < CHUNKS)
        def _():
            start_own(chunk(2))

        @pl.when((i >= 1) & (i - 1 < CHUNKS))
        def _():
            project(chunk(-1))
            send_first(chunk(-1))

        @pl.when((i >= 2) & (i - 2 < CHUNKS))
        def _():
            send_second(chunk(-2))

        @pl.when(i >= 3)
        def _():
            finish(chunk(-3))

    @pl.loop(0, 5)
    def _(t):
        for i in range(2):
            @pl.when(sends_next(t))
            def _():
                to_next(t, i).wait_send()

            @pl.when(sends_side(t))
            def _():
                to_side(t, i).wait_send()

    @pl.when(sends_far)
    def _():
        for i in range(2):
            to_far(i).wait_send()

    @pl.loop(0, CHUNKS)
    def _(c):
        for copy in (*own(c), *relays(c)):
            copy.wait_send()
        for copy in sums(c):
            copy().wait_send()
        write(c).wait()


def per_device(queries, keys, values, doc_lengths, out_weight):
    rows, q_width = queries.shape[1:]
    kv_width = keys.shape[2]
    depth, columns = out_weight.shape
    ys = lax.axis_size("batch")
    heads = q_width // HEAD
    span = rows // CHUNKS
    bf16, f32 = jnp.bfloat16, jnp.float32
    anywhere = pl.BlockSpec(memory_space=pl.ANY)
    dma = pltpu.SemaphoreType.DMA
    return pl.pallas_call(
        kernel,
        out_shape=jax.ShapeDtypeStruct((1, rows, columns), bf16),
        in_specs=[anywhere, anywhere, anywhere, pl.BlockSpec(memory_space=pltpu.SMEM), anywhere],
        out_specs=anywhere,
        scratch_shapes=[
            pltpu.VMEM((rows, q_width), bf16),
            pltpu.VMEM((heads, HEAD, rows), bf16),
            pltpu.VMEM((10, 2, rows, kv_width), bf16),
            pltpu.VMEM((2, HEAD, rows), bf16),
            pltpu.VMEM((rows, rows), f32),
            pltpu.VMEM((1, rows), jnp.int32),
            pltpu.VMEM((heads, 1, rows), f32),
            pltpu.VMEM((heads, 1, rows), f32),
            pltpu.VMEM((heads, HEAD, rows), f32),
            pltpu.VMEM((CHUNKS, ys, span, depth), bf16),
            pltpu.VMEM((depth, columns), bf16),
            pltpu.VMEM((CHUNKS, ys, span, columns), bf16),
            pltpu.VMEM((CHUNKS, 2, span // 2, columns), bf16),
            pltpu.VMEM((CHUNKS, 2, span, columns), bf16),
            pltpu.VMEM((rows, columns), bf16),
            dma((4,)),
            dma((10, 2)),
            dma((5, 2)),
            dma((5, 2)),
            dma((2,)),
            dma((CHUNKS, 4)),
            dma((CHUNKS, 4)),
            dma((CHUNKS, 6)),
            dma((CHUNKS, 6)),
            dma((CHUNKS,)),
        ],
        compiler_params=pltpu.CompilerParams(
            collective_id=0, has_side_effects=True, vmem_limit_bytes=60 * 1024 * 1024
        ),
    )(queries, keys, values, doc_lengths, out_weight)


def solution(mesh):
    return jax.shard_map(
        per_device,
        mesh=mesh,
        in_specs=(
            P("batch", "seq", "heads"),
            P("batch", "seq", "heads"),
            P("batch", "seq", "heads"),
            P("batch", None),
            P("heads", "batch"),
        ),
        out_specs=P("heads", "seq", "batch"),
        check_vma=False,
    )
```

```python
import functools

import jax
import jax.numpy as jnp
from jax import lax
from jax.experimental import pallas as pl
from jax.experimental.pallas import tpu as pltpu
from jax.sharding import PartitionSpec as P

MESH = pl.DeviceIdType.MESH
HEAD = 128
DOCS = 16
CHUNKS = 8
LAG = 2
LOWEST = -1e30
SCALE = (HEAD ** -0.5) * 1.4426950408889634


def kernel(
    q_hbm, k_hbm, v_hbm, docs, w_hbm, out_hbm,
    qv, qt, kv, vt, bias, first, top, total, shrink, raw, soft, acc, gathered, weight, partial, near, final, outv,
    load_sem, kv_recv, next_send, side_send, far_send, ag_send, ag_recv, rs_send, rs_recv, out_sem,
):
    s = lax.axis_index("seq")
    x = lax.axis_index("heads")
    y = lax.axis_index("batch")
    seqs, xs, ys = lax.axis_size("seq"), lax.axis_size("heads"), lax.axis_size("batch")
    z = s // 2
    odd = s % 2
    rows = qv.shape[0]
    heads = qt.shape[0]
    half = rows // 2
    span = rows // CHUNKS
    part = span // 2
    right, left, across = (x + 1) % xs, (x + xs - 1) % xs, (x + 2) % xs
    up, down = (y + 1) % ys, (y + ys - 1) % ys

    def remote(src, dst, send, recv, **where):
        return pltpu.make_async_remote_copy(
            src_ref=src, dst_ref=dst, send_sem=send, recv_sem=recv, device_id=where, device_id_type=MESH
        )

    load_k = pltpu.make_async_copy(k_hbm.at[0], kv.at[0, 0], load_sem.at[0])
    load_v = pltpu.make_async_copy(v_hbm.at[0], kv.at[0, 1], load_sem.at[1])
    load_q = pltpu.make_async_copy(q_hbm.at[0], qv, load_sem.at[2])
    load_w = pltpu.make_async_copy(w_hbm, weight, load_sem.at[3])
    load_k.start()
    load_v.start()
    load_q.start()
    load_w.start()

    barrier = pltpu.get_barrier_semaphore()
    for by in (1, 2, seqs - 2, seqs - 1):
        pl.semaphore_signal(barrier, inc=1, device_id={"seq": (s + by) % seqs}, device_id_type=MESH)
    for peer in (right, left):
        pl.semaphore_signal(barrier, inc=1, device_id={"heads": peer}, device_id_type=MESH)
    for peer in (up, down):
        pl.semaphore_signal(barrier, inc=1, device_id={"batch": peer}, device_id_type=MESH)
    pl.semaphore_wait(barrier, 8)

    def to_next(t, i):
        slot = jnp.minimum(2 * t + 2, 8)
        return remote(
            kv.at[2 * t, i], kv.at[slot, i], next_send.at[t, i], kv_recv.at[slot, i],
            seq=jnp.minimum(s + 2, seqs - 1),
        )

    def to_side(t, i):
        slot = jnp.maximum(2 * t + 1 - 2 * odd, 0)
        return remote(
            kv.at[2 * t, i], kv.at[slot, i], side_send.at[t, i], kv_recv.at[slot, i], seq=s + 1 - 2 * odd
        )

    def to_far(i):
        return remote(
            kv.at[8, i, half:], kv.at[9, i, half:], far_send.at[i], kv_recv.at[9, i], seq=jnp.minimum(s + 1, seqs - 1)
        )

    def sends_next(t):
        return (z >= t) & (t <= 3) & (s + 2 < seqs)

    def sends_side(t):
        return (z >= t) & (t >= odd) & (t <= 3 + odd)

    sends_far = (z >= 4) & (s + 1 < seqs)

    def forward(t, i):
        @pl.when(sends_next(t))
        def _():
            to_next(t, i).start()

        @pl.when(sends_side(t))
        def _():
            to_side(t, i).start()

        @pl.when(sends_far & (t == 4))
        def _():
            to_far(i).start()

    def arrived(slot, i):
        remote(kv.at[slot, i], kv.at[slot, i], next_send.at[0, i], kv_recv.at[slot, i], seq=s).wait_recv()

    load_k.wait()
    forward(0, 0)
    load_v.wait()
    forward(0, 1)

    q_pos = s * rows + lax.broadcasted_iota(jnp.int32, (1, rows), 1)
    starts = jnp.zeros((1, rows), jnp.int32)
    ended = jnp.int32(0)
    for d in range(DOCS):
        length = docs[0, d]
        ended = ended + length
        starts = starts + jnp.where(q_pos >= ended, length, 0)
    first[...] = starts
    top[...] = jnp.full(top.shape, LOWEST, jnp.float32)
    total[...] = jnp.zeros(total.shape, jnp.float32)

    load_q.wait()

    @pl.loop(0, heads)
    def _(h):
        qt[h] = qv[:, pl.ds(pl.multiple_of(h * HEAD, HEAD), HEAD)].T
        acc[h] = jnp.zeros((HEAD, rows), jnp.float32)

    def attend(slot, low, columns):
        count = rows - low
        for g in range(2):
            vt[g, :, :count] = kv[slot, 1, low:, g * HEAD : (g + 1) * HEAD].T
        k_pos = (s - slot) * rows + low + lax.broadcasted_iota(jnp.int32, (count, columns), 0)
        q_all = s * rows + lax.broadcasted_iota(jnp.int32, (count, columns), 1)
        seen = (k_pos >= first[:, :columns]) & (k_pos <= q_all)
        bias[:count, :columns] = jnp.where(seen, 0.0, LOWEST)

        def score(h):
            g = h // (heads // 2)
            keys = kv[slot, 0, low:, g * HEAD : (g + 1) * HEAD]
            scores = jnp.dot(keys, qt[h, :, :columns], preferred_element_type=jnp.float32)
            scores = scores + bias[:count, :columns]
            raw[h, :count, :columns] = scores
            before = top[h, :, :columns]
            now = jnp.maximum(before, jnp.max(scores, axis=0, keepdims=True))
            shrink[h, :, :columns] = jnp.exp2((before - now) * SCALE)
            top[h, :, :columns] = now

        def weigh(h):
            weights = jnp.exp2((raw[h, :count, :columns] - top[h, :, :columns]) * SCALE)
            total[h, :, :columns] = total[h, :, :columns] * shrink[h, :, :columns] + jnp.sum(
                weights, axis=0, keepdims=True
            )
            soft[h, :count, :columns] = weights.astype(jnp.bfloat16)

        def mix(h):
            g = h // (heads // 2)
            summed = jnp.dot(vt[g, :, :count], soft[h, :count, :columns], preferred_element_type=jnp.float32)
            acc[h, :, :columns] = acc[h, :, :columns] * shrink[h, :, :columns] + summed

        for i in range(heads + 2 * LAG):
            if i < heads:
                score(i)
            if 0 <= i - LAG < heads:
                weigh(i - LAG)
            if 0 <= i - 2 * LAG < heads:
                mix(i - 2 * LAG)

    @pl.loop(0, 9)
    def _(n):
        swapped = n + 2 * (n % 2) - 1
        slot = jnp.where((odd == 1) | (n == 0), n, swapped)

        @pl.when(s >= slot)
        def _():
            @pl.when(n >= 1)
            def _():
                for i in range(2):
                    arrived(slot, i)

                    @pl.when(slot % 2 == 0)
                    def _():
                        forward(slot // 2, i)

            attend(slot, 0, rows)

    @pl.when(s >= 9)
    def _():
        for i in range(2):
            remote(
                kv.at[9, i, half:], kv.at[9, i, half:], far_send.at[i], kv_recv.at[9, i], seq=s
            ).wait_recv()
        attend(9, half, half)

    @pl.loop(0, heads)
    def _(h):
        done = acc[h] * (1.0 / total[h])
        turned = done.T.astype(jnp.bfloat16)
        for c in range(CHUNKS):
            gathered[c, y, :, pl.ds(pl.multiple_of(h * HEAD, HEAD), HEAD)] = turned[c * span : (c + 1) * span]

    def own(c):
        return (
            remote(gathered.at[c, y], gathered.at[c, y], ag_send.at[c, 0], ag_recv.at[c, 0], batch=up),
            remote(gathered.at[c, y], gathered.at[c, y], ag_send.at[c, 1], ag_recv.at[c, 1], batch=down),
        )

    def from_neighbours(c):
        return (
            remote(gathered.at[c, down], gathered.at[c, down], ag_send.at[c, 0], ag_recv.at[c, 0], batch=up),
            remote(gathered.at[c, up], gathered.at[c, up], ag_send.at[c, 1], ag_recv.at[c, 1], batch=down),
        )

    def relays(c):
        a, b = gathered.at[c, down, :part], gathered.at[c, up, part:]
        return (
            remote(a, a, ag_send.at[c, 2], ag_recv.at[c, 2], batch=up),
            remote(b, b, ag_send.at[c, 3], ag_recv.at[c, 3], batch=down),
        )

    def from_far(c):
        opposite = (y + 2) % ys
        a, b = gathered.at[c, opposite, :part], gathered.at[c, opposite, part:]
        return (
            remote(a, a, ag_send.at[c, 2], ag_recv.at[c, 2], batch=up),
            remote(b, b, ag_send.at[c, 3], ag_recv.at[c, 3], batch=down),
        )

    def sums(c):
        table = (
            (partial.at[c, across, :part], near.at[c, 0], right),
            (partial.at[c, across, part:], near.at[c, 1], left),
            (partial.at[c, right, part:], final.at[c, 0, part:], right),
            (partial.at[c, left, :part], final.at[c, 1, :part], left),
            (partial.at[c, right, :part], final.at[c, 0, :part], right),
            (partial.at[c, left, part:], final.at[c, 1, part:], left),
        )
        return [
            functools.partial(remote, src, dst, rs_send.at[c, i], rs_recv.at[c, i], heads=to)
            for i, (src, dst, to) in enumerate(table)
        ]

    def start_own(c):
        for copy in own(c):
            copy.start()

    def relay(c):
        for arriving, onward in zip(from_neighbours(c), relays(c)):
            arriving.wait_recv()
            onward.start()

    wide = 512

    def project(c):
        for arriving in from_far(c):
            arriving.wait_recv()
        lhs = gathered[c].reshape(ys * span, -1)

        @pl.loop(0, weight.shape[1] // wide)
        def _(n):
            columns = pl.ds(pl.multiple_of(n * wide, wide), wide)
            product = jnp.dot(lhs, weight[:, columns], preferred_element_type=jnp.float32)
            partial[c, :, :, columns] = product.astype(jnp.bfloat16).reshape(ys, span, wide)

    def send_first(c):
        for copy in sums(c)[:4]:
            copy().start()

    def send_second(c):
        copies = sums(c)
        copies[0]().wait_recv()
        partial[c, right, :part] = (
            partial[c, right, :part].astype(jnp.float32) + near[c, 0].astype(jnp.float32)
        ).astype(jnp.bfloat16)
        copies[4]().start()
        copies[1]().wait_recv()
        partial[c, left, part:] = (
            partial[c, left, part:].astype(jnp.float32) + near[c, 1].astype(jnp.float32)
        ).astype(jnp.bfloat16)
        copies[5]().start()

    def write(c):
        return pltpu.make_async_copy(
            outv.at[pl.ds(pl.multiple_of(c * span, span), span)],
            out_hbm.at[0, pl.ds(pl.multiple_of(c * span, span), span)],
            out_sem.at[c],
        )

    def finish(c):
        copies = sums(c)
        for i in range(2, 6):
            copies[i]().wait_recv()
        value = (
            partial[c, x].astype(jnp.float32)
            + final[c, 0].astype(jnp.float32)
            + final[c, 1].astype(jnp.float32)
        )
        outv[pl.ds(pl.multiple_of(c * span, span), span)] = value.astype(jnp.bfloat16)
        write(c).start()

    start_own(0)
    start_own(1)
    load_w.wait()

    @pl.loop(0, CHUNKS + 3)
    def _(i):
        def chunk(by):
            return jnp.clip(i + by, 0, CHUNKS - 1)

        @pl.when(i < CHUNKS)
        def _():
            relay(chunk(0))

        @pl.when(i + 2 < CHUNKS)
        def _():
            start_own(chunk(2))

        @pl.when((i >= 1) & (i - 1 < CHUNKS))
        def _():
            project(chunk(-1))
            send_first(chunk(-1))

        @pl.when((i >= 2) & (i - 2 < CHUNKS))
        def _():
            send_second(chunk(-2))

        @pl.when(i >= 3)
        def _():
            finish(chunk(-3))

    @pl.loop(0, 5)
    def _(t):
        for i in range(2):
            @pl.when(sends_next(t))
            def _():
                to_next(t, i).wait_send()

            @pl.when(sends_side(t))
            def _():
                to_side(t, i).wait_send()

    @pl.when(sends_far)
    def _():
        for i in range(2):
            to_far(i).wait_send()

    @pl.loop(0, CHUNKS)
    def _(c):
        for copy in (*own(c), *relays(c)):
            copy.wait_send()
        for copy in sums(c):
            copy().wait_send()
        write(c).wait()


def per_device(queries, keys, values, doc_lengths, out_weight):
    rows, q_width = queries.shape[1:]
    kv_width = keys.shape[2]
    depth, columns = out_weight.shape
    ys = lax.axis_size("batch")
    heads = q_width // HEAD
    span = rows // CHUNKS
    bf16, f32 = jnp.bfloat16, jnp.float32
    anywhere = pl.BlockSpec(memory_space=pl.ANY)
    dma = pltpu.SemaphoreType.DMA
    return pl.pallas_call(
        kernel,
        out_shape=jax.ShapeDtypeStruct((1, rows, columns), bf16),
        in_specs=[anywhere, anywhere, anywhere, pl.BlockSpec(memory_space=pltpu.SMEM), anywhere],
        out_specs=anywhere,
        scratch_shapes=[
            pltpu.VMEM((rows, q_width), bf16),
            pltpu.VMEM((heads, HEAD, rows), bf16),
            pltpu.VMEM((10, 2, rows, kv_width), bf16),
            pltpu.VMEM((2, HEAD, rows), bf16),
            pltpu.VMEM((rows, rows), f32),
            pltpu.VMEM((1, rows), jnp.int32),
            pltpu.VMEM((heads, 1, rows), f32),
            pltpu.VMEM((heads, 1, rows), f32),
            pltpu.VMEM((heads, 1, rows), f32),
            pltpu.VMEM((heads, rows, rows), f32),
            pltpu.VMEM((heads, rows, rows), bf16),
            pltpu.VMEM((heads, HEAD, rows), f32),
            pltpu.VMEM((CHUNKS, ys, span, depth), bf16),
            pltpu.VMEM((depth, columns), bf16),
            pltpu.VMEM((CHUNKS, ys, span, columns), bf16),
            pltpu.VMEM((CHUNKS, 2, span // 2, columns), bf16),
            pltpu.VMEM((CHUNKS, 2, span, columns), bf16),
            pltpu.VMEM((rows, columns), bf16),
            dma((4,)),
            dma((10, 2)),
            dma((5, 2)),
            dma((5, 2)),
            dma((2,)),
            dma((CHUNKS, 4)),
            dma((CHUNKS, 4)),
            dma((CHUNKS, 6)),
            dma((CHUNKS, 6)),
            dma((CHUNKS,)),
        ],
        compiler_params=pltpu.CompilerParams(
            collective_id=0, has_side_effects=True, vmem_limit_bytes=60 * 1024 * 1024
        ),
    )(queries, keys, values, doc_lengths, out_weight)


def solution(mesh):
    return jax.shard_map(
        per_device,
        mesh=mesh,
        in_specs=(
            P("batch", "seq", "heads"),
            P("batch", "seq", "heads"),
            P("batch", "seq", "heads"),
            P("batch", None),
            P("heads", "batch"),
        ),
        out_specs=P("heads", "seq", "batch"),
        check_vma=False,
    )
```

```python
import functools

import jax
import jax.numpy as jnp
from jax import lax
from jax.experimental import pallas as pl
from jax.experimental.pallas import tpu as pltpu
from jax.sharding import PartitionSpec as P

MESH = pl.DeviceIdType.MESH
HEAD = 128
DOCS = 16
LAG = 2
EARLY = ((0, 0, 64), (0, 64, 64))
CHUNKS = ((0, 16), (16, 32), (48, 48), (96, 32), (128, 64), (192, 64))
LOWEST = -1e30
SCALE = (HEAD ** -0.5) * 1.4426950408889634


def kernel(
    q_hbm, k_hbm, v_hbm, docs, w_hbm, out_hbm,
    qv, qt, kv, vt, bias, first, top, total, shrink, raw, soft, acc, gathered, weight, partial, near, final, outv,
    load_sem, kv_recv, next_send, side_send, far_send, wrap_send, ag_send, ag_recv, rs_send, rs_recv, out_sem,
):
    s = lax.axis_index("seq")
    x = lax.axis_index("heads")
    y = lax.axis_index("batch")
    seqs, xs, ys = lax.axis_size("seq"), lax.axis_size("heads"), lax.axis_size("batch")
    z = s // 2
    odd = s % 2
    rows = qv.shape[0]
    heads = acc.shape[0]
    half = rows // 2
    right, left, across = (x + 1) % xs, (x + xs - 1) % xs, (x + 2) % xs
    up, down, opposite = (y + 1) % ys, (y + ys - 1) % ys, (y + 2) % ys

    def remote(src, dst, send, recv, **where):
        return pltpu.make_async_remote_copy(
            src_ref=src, dst_ref=dst, send_sem=send, recv_sem=recv, device_id=where, device_id_type=MESH
        )

    def load(g, i):
        src = (k_hbm, v_hbm)[i]
        return pltpu.make_async_copy(
            src.at[0, :, g * HEAD : (g + 1) * HEAD], kv.at[0, g, i], load_sem.at[2 * g + i]
        )

    load_q = pltpu.make_async_copy(q_hbm.at[0], qv, load_sem.at[4])
    load_w = pltpu.make_async_copy(w_hbm, weight, load_sem.at[5])
    for g in range(2):
        for i in range(2):
            load(g, i).start()
    load_q.start()
    load_w.start()

    barrier = pltpu.get_barrier_semaphore()
    for by in (1, 2, 6, 10, seqs - 2, seqs - 1):
        pl.semaphore_signal(barrier, inc=1, device_id={"seq": (s + by) % seqs}, device_id_type=MESH)
    for peer in (right, left):
        pl.semaphore_signal(barrier, inc=1, device_id={"heads": peer}, device_id_type=MESH)
    for peer in (up, down):
        pl.semaphore_signal(barrier, inc=1, device_id={"batch": peer}, device_id_type=MESH)
    pl.semaphore_wait(barrier, 10)

    def to_next(t, g, i):
        slot = jnp.minimum(2 * t + 2, 8)
        return remote(
            kv.at[2 * t, g, i], kv.at[slot, g, i], next_send.at[jnp.minimum(t, 3), g, i], kv_recv.at[slot, g, i],
            seq=jnp.minimum(s + 2, seqs - 1),
        )

    def to_side(t, g, i):
        slot = jnp.maximum(2 * t + 1 - 2 * odd, 0)
        return remote(
            kv.at[2 * t, g, i], kv.at[slot, g, i], side_send.at[t, g, i], kv_recv.at[slot, g, i],
            seq=s + 1 - 2 * odd,
        )

    def to_far(g, i):
        return remote(
            kv.at[8, g, i, half:], kv.at[9, g, i, half:], far_send.at[g, i], kv_recv.at[9, g, i],
            seq=jnp.minimum(s + 1, seqs - 1),
        )

    def to_wrap(i):
        return remote(kv.at[0, 1, i], kv.at[10, 1, i], wrap_send.at[0, i], kv_recv.at[10, 1, i], seq=(s + 10) % seqs)

    def to_back(i):
        return remote(
            kv.at[10, 1, i], kv.at[8, 1, i], wrap_send.at[1, i], kv_recv.at[8, 1, i], seq=(s + seqs - 2) % seqs
        )

    def to_corner(i):
        return remote(
            kv.at[10, 1, i, half:], kv.at[9, 1, i, half:], wrap_send.at[2, i], kv_recv.at[9, 1, i],
            seq=jnp.maximum(s - 1, 0),
        )

    def sends_next(t, g):
        return (z >= t) & (t <= 3 - g) & (s + 2 < seqs)

    def sends_side(t):
        return (z >= t) & (t >= odd) & (t <= 3 + odd)

    def sends_far(g):
        return (z >= 4) & (s + 1 < seqs) & (g * odd == 0)

    sends_wrap = s < 8
    transit = (s >= 10) | (s < 2)
    corner = (s >= 10) & (odd == 1)

    def forward(t, g, i):
        @pl.when(sends_next(t, g))
        def _():
            to_next(t, g, i).start()

        @pl.when(sends_side(t))
        def _():
            to_side(t, g, i).start()

        @pl.when(sends_far(g) & (t == 4))
        def _():
            to_far(g, i).start()

    def arrived(slot, g, i):
        remote(kv.at[slot, g, i], kv.at[slot, g, i], next_send.at[0, 0, i], kv_recv.at[slot, g, i], seq=s).wait_recv()

    for i in range(2):
        load(0, i).wait()
        forward(0, 0, i)
    for i in range(2):
        load(1, i).wait()

        @pl.when(sends_wrap)
        def _():
            to_wrap(i).start()

        @pl.when(z == 0)
        def _():
            forward(0, 1, i)

    q_pos = s * rows + lax.broadcasted_iota(jnp.int32, (1, rows), 1)
    starts = jnp.zeros((1, rows), jnp.int32)
    ended = jnp.int32(0)
    for d in range(DOCS):
        length = docs[0, d]
        ended = ended + length
        starts = starts + jnp.where(q_pos >= ended, length, 0)
    first[...] = starts

    load_q.wait()

    @pl.loop(0, 2 * heads)
    def _(h):
        qt[h] = qv[:, pl.ds(pl.multiple_of(h * HEAD, HEAD), HEAD)].T

    def attend(slot, g, low, columns):
        count = rows - low
        keys = kv.at[slot, g, 0]
        queries = qt.at[pl.ds(g * heads, heads)]
        vt[:, :count] = kv[slot, g, 1, low:].T
        k_pos = (s - slot) * rows + low + lax.broadcasted_iota(jnp.int32, (count, columns), 0)
        q_all = s * rows + lax.broadcasted_iota(jnp.int32, (count, columns), 1)
        seen = (k_pos >= first[:, :columns]) & (k_pos <= q_all)
        bias[:count, :columns] = jnp.where(seen, 0.0, LOWEST)

        def score(h):
            scores = jnp.dot(keys[low:], queries[h, :, :columns], preferred_element_type=jnp.float32)
            scores = scores + bias[:count, :columns]
            raw[h, :count, :columns] = scores
            before = top[h, :, :columns]
            now = jnp.maximum(before, jnp.max(scores, axis=0, keepdims=True))
            shrink[h, :, :columns] = jnp.exp2((before - now) * SCALE)
            top[h, :, :columns] = now

        def weigh(h):
            weights = jnp.exp2((raw[h, :count, :columns] - top[h, :, :columns]) * SCALE)
            total[h, :, :columns] = total[h, :, :columns] * shrink[h, :, :columns] + jnp.sum(
                weights, axis=0, keepdims=True
            )
            soft[h, :count, :columns] = weights.astype(jnp.bfloat16)

        def mix(h):
            summed = jnp.dot(vt[:, :count], soft[h, :count, :columns], preferred_element_type=jnp.float32)
            acc[h, :, :columns] = acc[h, :, :columns] * shrink[h, :, :columns] + summed

        for i in range(heads + 2 * LAG):
            if i < heads:
                score(i)
            if 0 <= i - LAG < heads:
                weigh(i - LAG)
            if 0 <= i - 2 * LAG < heads:
                mix(i - 2 * LAG)

    width = gathered.shape[3]
    middle = width // 2
    items = list(EARLY)
    covers = []
    for o, n in CHUNKS:
        mine = [(g, o, n) for g in range(2) if g == 1 or o >= half]
        covers.append(range(len(items), len(items) + len(mine)))
        items += mine

    def copies_of(k, holder, far):
        g, o, n = items[k]
        a = gathered.at[g, holder[0], o : o + n]
        b = gathered.at[g, holder[1], o : o + n]
        if far:
            a, b = a.at[:, :middle], b.at[:, middle:]
        return (
            remote(a, a, ag_send.at[k, 2 * far], ag_recv.at[k, 2 * far], batch=up),
            remote(b, b, ag_send.at[k, 2 * far + 1], ag_recv.at[k, 2 * far + 1], batch=down),
        )

    def start_own(k):
        for copy in copies_of(k, (y, y), 0):
            copy.start()

    def relay(k):
        for arriving, onward in zip(copies_of(k, (down, up), 0), copies_of(k, (down, up), 1)):
            arriving.wait_recv()
            onward.start()

    def settle(k):
        for arriving in copies_of(k, (opposite, opposite), 1):
            arriving.wait_recv()

    def normalize(g, low):
        for h in range(heads):
            done = acc[h, :, low : low + half] * (1.0 / total[h, :, low : low + half])
            gathered[g, y, low : low + half, h * HEAD : (h + 1) * HEAD] = done.T.astype(jnp.bfloat16)

    @pl.loop(0, 2)
    def _(g):
        top[...] = jnp.full(top.shape, LOWEST, jnp.float32)
        total[...] = jnp.zeros(total.shape, jnp.float32)

        @pl.loop(0, heads)
        def _(h):
            acc[h] = jnp.zeros(acc.shape[1:], jnp.float32)

        @pl.loop(0, 9)
        def _(n):
            swapped = n + 2 * (n % 2) - 1
            slot = jnp.where((odd == 1) | (n == 0), n, jnp.clip(swapped, 0, 8))

            @pl.when(s >= slot)
            def _():
                @pl.when(n >= 1)
                def _():
                    for i in range(2):
                        arrived(slot, g, i)

                        @pl.when(slot % 2 == 0)
                        def _():
                            forward(slot // 2, g, i)

                    @pl.when((g == 0) & (slot == 2 * jnp.minimum(z, 3)))
                    def _():
                        for i in range(2):
                            forward(0, 1, i)

                attend(slot, g, 0, rows)

            for k, at in ((0, 4), (1, 7)):
                @pl.when((g == 1) & (n == at))
                def _():
                    relay(k)

        @pl.when((g == 0) & transit)
        def _():
            for i in range(2):
                arrived(10, 1, i)
                to_back(i).start()

                @pl.when(corner)
                def _():
                    to_corner(i).start()

        @pl.when(s >= 9)
        def _():
            for i in range(2):
                remote(
                    kv.at[9, g, i, half:], kv.at[9, g, i, half:], far_send.at[0, i], kv_recv.at[9, g, i], seq=s
                ).wait_recv()
            attend(9, g, half, half)

        normalize(g, 0)

        @pl.when(g == 0)
        def _():
            for k in range(len(EARLY)):
                start_own(k)

        @pl.when(g == 1)
        def _():
            for c in range(2):
                for k in covers[c]:
                    start_own(k)

        normalize(g, half)

    part = weight.shape[1] // 2
    wide = 512

    def sums(c):
        o, n = CHUNKS[c]
        some = slice(o, o + n)
        table = (
            (partial.at[across, some, :part], near.at[0, some], right),
            (partial.at[across, some, part:], near.at[1, some], left),
            (partial.at[right, some, part:], final.at[0, some, part:], right),
            (partial.at[left, some, :part], final.at[1, some, :part], left),
            (partial.at[right, some, :part], final.at[0, some, :part], right),
            (partial.at[left, some, part:], final.at[1, some, part:], left),
        )
        return [
            functools.partial(remote, src, dst, rs_send.at[c, i], rs_recv.at[c, i], heads=to)
            for i, (src, dst, to) in enumerate(table)
        ]

    def project(c):
        o, n = CHUNKS[c]
        for k in covers[c]:
            settle(k)
        lhs = jnp.concatenate([gathered[g, :, o : o + n].reshape(ys * n, width) for g in range(2)], axis=1)

        @pl.loop(0, weight.shape[1] // wide)
        def _(m):
            columns = pl.ds(pl.multiple_of(m * wide, wide), wide)
            product = jnp.dot(lhs, weight[:, columns], preferred_element_type=jnp.float32)
            partial[:, o : o + n, columns] = product.astype(jnp.bfloat16).reshape(ys, n, wide)

    def send_first(c):
        for copy in sums(c)[:4]:
            copy().start()

    def send_second(c):
        o, n = CHUNKS[c]
        copies = sums(c)
        for i, to, low in ((0, right, 0), (1, left, part)):
            copies[i]().wait_recv()
            partial[to, o : o + n, low : low + part] = (
                partial[to, o : o + n, low : low + part].astype(jnp.float32)
                + near[i, o : o + n].astype(jnp.float32)
            ).astype(jnp.bfloat16)
            copies[4 + i]().start()

    def write(c):
        o, n = CHUNKS[c]
        return pltpu.make_async_copy(outv.at[o : o + n], out_hbm.at[0, o : o + n], out_sem.at[c])

    def finish(c):
        o, n = CHUNKS[c]
        copies = sums(c)
        for i in range(2, 6):
            copies[i]().wait_recv()
        value = (
            partial[x, o : o + n].astype(jnp.float32)
            + final[0, o : o + n].astype(jnp.float32)
            + final[1, o : o + n].astype(jnp.float32)
        )
        outv[o : o + n] = value.astype(jnp.bfloat16)
        write(c).start()

    load_w.wait()
    for k in range(len(EARLY)):
        settle(k)
    chunks = len(CHUNKS)
    for i in range(chunks + 3):
        if i < chunks:
            for k in covers[i]:
                relay(k)
        if i + 2 < chunks:
            for k in covers[i + 2]:
                start_own(k)
        if 0 <= i - 1 < chunks:
            project(i - 1)
            send_first(i - 1)
        if 0 <= i - 2 < chunks:
            send_second(i - 2)
        if i >= 3:
            finish(i - 3)

    @pl.loop(0, 5)
    def _(t):
        for g in range(2):
            for i in range(2):
                @pl.when(sends_next(t, g))
                def _():
                    to_next(t, g, i).wait_send()

                @pl.when(sends_side(t))
                def _():
                    to_side(t, g, i).wait_send()

    for i in range(2):
        for g in range(2):
            @pl.when(sends_far(g))
            def _():
                to_far(g, i).wait_send()

        @pl.when(sends_wrap)
        def _():
            to_wrap(i).wait_send()

        @pl.when(transit)
        def _():
            to_back(i).wait_send()

        @pl.when(corner)
        def _():
            to_corner(i).wait_send()

    for k in range(len(items)):
        for copy in (*copies_of(k, (y, y), 0), *copies_of(k, (down, up), 1)):
            copy.wait_send()
    for c in range(chunks):
        for copy in sums(c):
            copy().wait_send()
        write(c).wait()


def per_device(queries, keys, values, doc_lengths, out_weight):
    rows, q_width = queries.shape[1:]
    kv_heads = keys.shape[2] // HEAD
    depth, columns = out_weight.shape
    ys = lax.axis_size("batch")
    heads = q_width // HEAD // kv_heads
    items = len(EARLY) + len(CHUNKS) + sum(o >= rows // 2 for o, _ in CHUNKS)
    bf16, f32 = jnp.bfloat16, jnp.float32
    anywhere = pl.BlockSpec(memory_space=pl.ANY)
    dma = pltpu.SemaphoreType.DMA
    return pl.pallas_call(
        kernel,
        out_shape=jax.ShapeDtypeStruct((1, rows, columns), bf16),
        in_specs=[anywhere, anywhere, anywhere, pl.BlockSpec(memory_space=pltpu.SMEM), anywhere],
        out_specs=anywhere,
        scratch_shapes=[
            pltpu.VMEM((rows, q_width), bf16),
            pltpu.VMEM((kv_heads * heads, HEAD, rows), bf16),
            pltpu.VMEM((11, kv_heads, 2, rows, HEAD), bf16),
            pltpu.VMEM((HEAD, rows), bf16),
            pltpu.VMEM((rows, rows), f32),
            pltpu.VMEM((1, rows), jnp.int32),
            pltpu.VMEM((heads, 1, rows), f32),
            pltpu.VMEM((heads, 1, rows), f32),
            pltpu.VMEM((heads, 1, rows), f32),
            pltpu.VMEM((heads, rows, rows), f32),
            pltpu.VMEM((heads, rows, rows), bf16),
            pltpu.VMEM((heads, HEAD, rows), f32),
            pltpu.VMEM((kv_heads, ys, rows, heads * HEAD), bf16),
            pltpu.VMEM((depth, columns), bf16),
            pltpu.VMEM((ys, rows, columns), bf16),
            pltpu.VMEM((2, rows, columns // 2), bf16),
            pltpu.VMEM((2, rows, columns), bf16),
            pltpu.VMEM((rows, columns), bf16),
            dma((6,)),
            dma((11, 2, 2)),
            dma((4, 2, 2)),
            dma((5, 2, 2)),
            dma((2, 2)),
            dma((3, 2)),
            dma((items, 4)),
            dma((items, 4)),
            dma((len(CHUNKS), 6)),
            dma((len(CHUNKS), 6)),
            dma((len(CHUNKS),)),
        ],
        compiler_params=pltpu.CompilerParams(
            collective_id=0, has_side_effects=True, vmem_limit_bytes=60 * 1024 * 1024
        ),
    )(queries, keys, values, doc_lengths, out_weight)


def solution(mesh):
    return jax.shard_map(
        per_device,
        mesh=mesh,
        in_specs=(
            P("batch", "seq", "heads"),
            P("batch", "seq", "heads"),
            P("batch", "seq", "heads"),
            P("batch", None),
            P("heads", "batch"),
        ),
        out_specs=P("heads", "seq", "batch"),
        check_vma=False,
    )
```

```python
import functools

import jax
import jax.numpy as jnp
from jax import lax
from jax.experimental import pallas as pl
from jax.experimental.pallas import tpu as pltpu
from jax.sharding import PartitionSpec as P

MESH = pl.DeviceIdType.MESH
HEAD = 128
DOCS = 16
LAG = 3
EARLY = ((0, 64), (64, 64))
CHUNKS = tuple((32 * c, 32) for c in range(8))
LOWEST = -1e30
SCALE = (HEAD ** -0.5) * 1.4426950408889634


def kernel(
    q_hbm, k_hbm, v_hbm, docs, w_hbm, outv,
    qv, qt, kv, vt, bias, top, total, shrink, raw, soft, acc, gathered, weight, partial, near, final,
    load_sem, kv_recv, next_send, side_send, far_send, wrap_send, ag_send, ag_recv, rs_send, rs_recv,
):
    s = lax.axis_index("seq")
    x = lax.axis_index("heads")
    y = lax.axis_index("batch")
    seqs, xs, ys = lax.axis_size("seq"), lax.axis_size("heads"), lax.axis_size("batch")
    z = s // 2
    odd = s % 2
    rows = qv.shape[0]
    heads = acc.shape[0] // 2
    half = rows // 2
    right, left, across = (x + 1) % xs, (x + xs - 1) % xs, (x + 2) % xs
    up, down, opposite = (y + 1) % ys, (y + ys - 1) % ys, (y + 2) % ys

    def remote(src, dst, send, recv, **where):
        return pltpu.make_async_remote_copy(
            src_ref=src, dst_ref=dst, send_sem=send, recv_sem=recv, device_id=where, device_id_type=MESH
        )

    def load(g, i):
        src = (k_hbm, v_hbm)[i]
        return pltpu.make_async_copy(
            src.at[0, :, g * HEAD : (g + 1) * HEAD], kv.at[0, g, i], load_sem.at[2 * g + i]
        )

    load_q = pltpu.make_async_copy(q_hbm.at[0], qv, load_sem.at[4])
    load_w = pltpu.make_async_copy(w_hbm, weight, load_sem.at[5])
    for g in range(2):
        for i in range(2):
            load(g, i).start()
    load_q.start()
    load_w.start()

    barrier = pltpu.get_barrier_semaphore()
    for by in (1, 2, 6, 7, 9, 10, seqs - 2, seqs - 1):
        pl.semaphore_signal(barrier, inc=1, device_id={"seq": (s + by) % seqs}, device_id_type=MESH)
    for peer in (right, left):
        pl.semaphore_signal(barrier, inc=1, device_id={"heads": peer}, device_id_type=MESH)
    for peer in (up, down):
        pl.semaphore_signal(barrier, inc=1, device_id={"batch": peer}, device_id_type=MESH)
    pl.semaphore_wait(barrier, 12)

    def to_next(t, g, i):
        slot = jnp.minimum(2 * t + 2, 8)
        return remote(
            kv.at[2 * t, g, i], kv.at[slot, g, i], next_send.at[jnp.minimum(t, 3), g, i], kv_recv.at[slot, g, i],
            seq=jnp.minimum(s + 2, seqs - 1),
        )

    def to_side(t, g, i):
        slot = jnp.maximum(2 * t + 1 - 2 * odd, 0)
        return remote(
            kv.at[2 * t, g, i], kv.at[slot, g, i], side_send.at[t, g, i], kv_recv.at[slot, g, i],
            seq=s + 1 - 2 * odd,
        )

    def to_far(g, i):
        return remote(
            kv.at[8, g, i, half:], kv.at[9, g, i, half:], far_send.at[g, i], kv_recv.at[9, g, i],
            seq=jnp.minimum(s + 1, seqs - 1),
        )

    def to_jump(i):
        return remote(
            kv.at[0, 0, i, half:], kv.at[9, 0, i, half:], far_send.at[2, i], kv_recv.at[9, 0, i], seq=(s + 9) % seqs
        )

    def to_wrap(i):
        return remote(kv.at[0, 1, i], kv.at[10, 1, i], wrap_send.at[0, i], kv_recv.at[10, 1, i], seq=(s + 10) % seqs)

    def to_back(i):
        return remote(
            kv.at[10, 1, i], kv.at[8, 1, i], wrap_send.at[1, i], kv_recv.at[8, 1, i], seq=(s + seqs - 2) % seqs
        )

    def to_corner(i):
        return remote(
            kv.at[10, 1, i, half:], kv.at[9, 1, i, half:], wrap_send.at[2, i], kv_recv.at[9, 1, i],
            seq=jnp.maximum(s - 1, 0),
        )

    def sends_next(t, g):
        return (z >= t) & (t <= 3 - g) & (s + 2 < seqs)

    def sends_side(t):
        return (z >= t) & (t >= odd) & (t <= 3 + odd)

    sends_far = (z >= 4) & (odd == 0)
    sends_jump = (s < 6) & (odd == 1)

    sends_wrap = s < 8
    transit = (s >= 10) | (s < 2)
    corner = (s >= 10) & (odd == 1)

    def forward(t, g, i):
        @pl.when(sends_next(t, g))
        def _():
            to_next(t, g, i).start()

        @pl.when(sends_side(t))
        def _():
            to_side(t, g, i).start()

        @pl.when(sends_far & (t == 4))
        def _():
            to_far(g, i).start()

    def arrived(slot, g, i):
        remote(kv.at[slot, g, i], kv.at[slot, g, i], next_send.at[0, 0, 0], kv_recv.at[slot, g, i], seq=s).wait_recv()

    for g in range(2):
        for i in range(2):
            load(g, i).wait()
            forward(0, g, i)

    for i in range(2):
        @pl.when(sends_wrap)
        def _():
            to_wrap(i).start()

        @pl.when(sends_jump)
        def _():
            to_jump(i).start()

    q_pos = s * rows + lax.broadcasted_iota(jnp.int32, (1, rows), 1)
    starts = jnp.zeros((1, rows), jnp.int32)
    ended = jnp.int32(0)
    for d in range(DOCS):
        length = docs[0, d]
        ended = ended + length
        starts = starts + jnp.where(q_pos >= ended, length, 0)

    @pl.loop(0, 10)
    def _(slot):
        k_pos = (s - slot) * rows + lax.broadcasted_iota(jnp.int32, (rows, rows), 0)
        q_all = s * rows + lax.broadcasted_iota(jnp.int32, (rows, rows), 1)
        bias[slot] = jnp.where((k_pos >= starts) & (k_pos <= q_all), 0.0, LOWEST)

    vt[HEAD:] = jnp.ones((vt.shape[0] - HEAD, rows), jnp.bfloat16)
    load_q.wait()

    @pl.loop(0, 2 * heads)
    def _(h):
        qt[h] = qv[:, pl.ds(pl.multiple_of(h * HEAD, HEAD), HEAD)].T

    def attend(slot, g, low, columns):
        count = rows - low
        keys = kv.at[slot, g, 0]
        mine = pl.ds(g * heads, heads)
        queries, high, sums_of, mixed = qt.at[mine], top.at[mine], total.at[mine], acc.at[mine]
        shift = bias.at[slot]
        vt[:HEAD, :count] = kv[slot, g, 1, low:].T

        def score(h):
            scores = jnp.dot(keys[low:], queries[h, :, :columns], preferred_element_type=jnp.float32)
            scores = scores + shift[low:, :columns]
            raw[h, :count, :columns] = scores
            before = high[h, :, :columns]
            now = jnp.maximum(before, jnp.max(scores, axis=0, keepdims=True))
            shrink[h, :, :columns] = jnp.exp2((before - now) * SCALE)
            high[h, :, :columns] = now

        def weigh(h):
            weights = jnp.exp2((raw[h, :count, :columns] - high[h, :, :columns]) * SCALE)
            soft[h, :count, :columns] = weights.astype(jnp.bfloat16)

        def mix(h):
            summed = jnp.dot(vt[:, :count], soft[h, :count, :columns], preferred_element_type=jnp.float32)
            mixed[h, :, :columns] = mixed[h, :, :columns] * shrink[h, :, :columns] + summed[:HEAD]
            sums_of[h, :, :columns] = sums_of[h, :, :columns] * shrink[h, :, :columns] + summed[HEAD : HEAD + 1]

        for i in range(heads + 2 * LAG):
            if i < heads:
                score(i)
            if 0 <= i - LAG < heads:
                weigh(i - LAG)
            if 0 <= i - 2 * LAG < heads:
                mix(i - 2 * LAG)

    middle = gathered.shape[3] // 2
    early = sum(n for _, n in EARLY)
    items = [(slice(1, 2), o, n) for o, n in EARLY]
    items += [(slice(0, 1) if o < early else slice(0, 2), o, n) for o, n in CHUNKS]

    def copies_of(k, holder, far):
        groups, o, n = items[k]
        a = gathered.at[groups, holder[0], o : o + n]
        b = gathered.at[groups, holder[1], o : o + n]
        if far:
            a, b = a.at[:, :, :middle], b.at[:, :, middle:]
        return (
            remote(a, a, ag_send.at[k, 2 * far], ag_recv.at[k, 2 * far], batch=up),
            remote(b, b, ag_send.at[k, 2 * far + 1], ag_recv.at[k, 2 * far + 1], batch=down),
        )

    def start_own(k):
        for copy in copies_of(k, (y, y), 0):
            copy.start()

    def relay(k):
        for arriving, copy in zip(copies_of(k, (down, up), 0), copies_of(k, (down, up), 1)):
            arriving.wait_recv()
            copy.start()

    def settle(k):
        for arriving in copies_of(k, (opposite, opposite), 1):
            arriving.wait_recv()

    def normalize(g, low):
        mine = pl.ds(g * heads, heads)
        for h in range(heads):
            done = acc.at[mine][h, :, low : low + half] * (1.0 / total.at[mine][h, :, low : low + half])
            gathered[g, y, low : low + half, h * HEAD : (h + 1) * HEAD] = done.T.astype(jnp.bfloat16)

    top[...] = jnp.full(top.shape, LOWEST, jnp.float32)
    total[...] = jnp.zeros(total.shape, jnp.float32)

    @pl.loop(0, 2 * heads)
    def _(h):
        acc[h] = jnp.zeros(acc.shape[1:], jnp.float32)

    @pl.loop(0, 14)
    def _(m):
        n, g = m // 2, m % 2
        t = (n + 1) // 2
        lane = n % 2 == 0
        here = (z >= t) & (n >= 1) & (n <= 8)
        side = n - 2 * (1 - odd)

        @pl.when(here)
        def _():
            arrived(2 * t, 1 - n % 2, g)
            forward(t, 1 - n % 2, g)

        slot = jnp.where(lane, n, jnp.maximum(side, 0))
        taken = jnp.where(lane, (n <= 8) & (z >= t), (side >= 1) & (side <= 7) & (s >= side))

        @pl.when(taken)
        def _():
            @pl.when(n % 2 == 1)
            def _():
                for i in range(2):
                    arrived(slot, g, i)

            attend(slot, g, 0, rows)

        @pl.when((m == 9) & transit)
        def _():
            for i in range(2):
                arrived(10, 1, i)
                to_back(i).start()

                @pl.when(corner)
                def _():
                    to_corner(i).start()

    @pl.loop(0, 2)
    def _(r):
        g = 1 - r

        @pl.loop(0, 5)
        def _(q):
            lane = q == 2
            n = jnp.where(q == 0, 7, jnp.where(lane, 8, 9))
            side = n - 2 * (1 - odd)

            @pl.when(lane & (z >= 4))
            def _():
                for i in range(2):
                    arrived(8, g, i)
                    forward(4, g, i)

            slot = jnp.where(lane, 8, side)

            @pl.when((q % 4 != 1) & (q < 4) & jnp.where(lane, z >= 4, (side <= 7) & (s >= side)))
            def _():
                @pl.when(q != 2)
                def _():
                    for i in range(2):
                        arrived(jnp.minimum(slot, 9), g, i)

                attend(jnp.minimum(slot, 8), g, 0, rows)

            @pl.when((q == 1 + 3 * odd) & (s >= 9))
            def _():
                for i in range(2):
                    remote(
                        kv.at[9, g, i, half:], kv.at[9, g, i, half:], far_send.at[0, i], kv_recv.at[9, g, i], seq=s
                    ).wait_recv()
                attend(9, g, half, half)

        normalize(g, 0)

        @pl.when(r == 0)
        def _():
            start_own(0)

        @pl.when(r == 1)
        def _():
            start_own(2)

        normalize(g, half)

        @pl.when(r == 0)
        def _():
            start_own(1)

    part = weight.shape[1] // 2
    wide = 512

    def sums(c):
        o, n = CHUNKS[c]
        some = slice(o, o + n)
        table = (
            (partial.at[across, some, :part], near.at[0, some], right),
            (partial.at[across, some, part:], near.at[1, some], left),
            (partial.at[right, some, part:], final.at[0, some, part:], right),
            (partial.at[left, some, :part], final.at[1, some, :part], left),
            (partial.at[right, some, :part], final.at[0, some, :part], right),
            (partial.at[left, some, part:], final.at[1, some, part:], left),
        )
        return [
            functools.partial(remote, src, dst, rs_send.at[c, i], rs_recv.at[c, i], heads=to)
            for i, (src, dst, to) in enumerate(table)
        ]

    def project(c):
        o, n = CHUNKS[c]
        for k, (e, many) in enumerate(EARLY):
            if o == e:
                settle(k)
        settle(len(EARLY) + c)
        lhs = jnp.concatenate([gathered[g, :, o : o + n].reshape(ys * n, -1) for g in range(2)], axis=1)

        @pl.loop(0, weight.shape[1] // wide)
        def _(m):
            columns = pl.ds(pl.multiple_of(m * wide, wide), wide)
            product = jnp.dot(lhs, weight[:, columns], preferred_element_type=jnp.float32)
            partial[:, o : o + n, columns] = product.astype(jnp.bfloat16).reshape(ys, n, wide)

    def send_first(c):
        for copy in sums(c)[:4]:
            copy().start()

    def send_second(c):
        o, n = CHUNKS[c]
        copies = sums(c)
        for i, to, low in ((0, right, 0), (1, left, part)):
            copies[i]().wait_recv()
            partial[to, o : o + n, low : low + part] = (
                partial[to, o : o + n, low : low + part].astype(jnp.float32)
                + near[i, o : o + n].astype(jnp.float32)
            ).astype(jnp.bfloat16)
            copies[4 + i]().start()

    def finish(c):
        o, n = CHUNKS[c]
        copies = sums(c)
        for i in range(2, 6):
            copies[i]().wait_recv()
        value = (
            partial[x, o : o + n].astype(jnp.float32)
            + final[0, o : o + n].astype(jnp.float32)
            + final[1, o : o + n].astype(jnp.float32)
        )
        outv[0, o : o + n] = value.astype(jnp.bfloat16)

    load_w.wait()
    chunks = len(CHUNKS)
    first_chunk = len(EARLY)
    relay(0)
    start_own(first_chunk + 1)
    relay(1)
    for i in range(chunks + 3):
        if i < chunks:
            relay(first_chunk + i)
        if i + 2 < chunks:
            start_own(first_chunk + i + 2)
        if 0 <= i - 1 < chunks:
            project(i - 1)
            send_first(i - 1)
        if 0 <= i - 2 < chunks:
            send_second(i - 2)
        if i >= 3:
            finish(i - 3)

    @pl.loop(0, 5)
    def _(t):
        for g in range(2):
            for i in range(2):
                @pl.when(sends_next(t, g))
                def _():
                    to_next(t, g, i).wait_send()

                @pl.when(sends_side(t))
                def _():
                    to_side(t, g, i).wait_send()

    for i in range(2):
        for g in range(2):
            @pl.when(sends_far)
            def _():
                to_far(g, i).wait_send()

        @pl.when(sends_jump)
        def _():
            to_jump(i).wait_send()

        @pl.when(sends_wrap)
        def _():
            to_wrap(i).wait_send()

        @pl.when(transit)
        def _():
            to_back(i).wait_send()

        @pl.when(corner)
        def _():
            to_corner(i).wait_send()

    for k in range(len(items)):
        for copy in (*copies_of(k, (y, y), 0), *copies_of(k, (down, up), 1)):
            copy.wait_send()
    for c in range(chunks):
        for copy in sums(c):
            copy().wait_send()


def per_device(queries, keys, values, doc_lengths, out_weight):
    rows, q_width = queries.shape[1:]
    kv_heads = keys.shape[2] // HEAD
    depth, columns = out_weight.shape
    ys = lax.axis_size("batch")
    heads = q_width // HEAD // kv_heads
    items = len(EARLY) + len(CHUNKS)
    bf16, f32 = jnp.bfloat16, jnp.float32
    anywhere = pl.BlockSpec(memory_space=pl.ANY)
    dma = pltpu.SemaphoreType.DMA
    held = pl.pallas_call(
        kernel,
        out_shape=pltpu.VMEM((1, rows, columns), bf16),
        in_specs=[anywhere, anywhere, anywhere, pl.BlockSpec(memory_space=pltpu.SMEM), anywhere],
        out_specs=pl.BlockSpec(memory_space=pltpu.VMEM),
        scratch_shapes=[
            pltpu.VMEM((rows, q_width), bf16),
            pltpu.VMEM((kv_heads * heads, HEAD, rows), bf16),
            pltpu.VMEM((11, kv_heads, 2, rows, HEAD), bf16),
            pltpu.VMEM((HEAD + 16, rows), bf16),
            pltpu.VMEM((10, rows, rows), f32),
            pltpu.VMEM((kv_heads * heads, 1, rows), f32),
            pltpu.VMEM((kv_heads * heads, 1, rows), f32),
            pltpu.VMEM((heads, 1, rows), f32),
            pltpu.VMEM((heads, rows, rows), f32),
            pltpu.VMEM((heads, rows, rows), bf16),
            pltpu.VMEM((kv_heads * heads, HEAD, rows), f32),
            pltpu.VMEM((kv_heads, ys, rows, heads * HEAD), bf16),
            pltpu.VMEM((depth, columns), bf16),
            pltpu.VMEM((ys, rows, columns), bf16),
            pltpu.VMEM((2, rows, columns // 2), bf16),
            pltpu.VMEM((2, rows, columns), bf16),
            dma((6,)),
            dma((11, 2, 2)),
            dma((4, 2, 2)),
            dma((5, 2, 2)),
            dma((3, 2)),
            dma((3, 2)),
            dma((items, 4)),
            dma((items, 4)),
            dma((len(CHUNKS), 6)),
            dma((len(CHUNKS), 6)),
        ],
        compiler_params=pltpu.CompilerParams(
            collective_id=0, has_side_effects=True, vmem_limit_bytes=60 * 1024 * 1024
        ),
    )(queries, keys, values, doc_lengths, out_weight)
    return held


def solution(mesh):
    return jax.shard_map(
        per_device,
        mesh=mesh,
        in_specs=(
            P("batch", "seq", "heads"),
            P("batch", "seq", "heads"),
            P("batch", "seq", "heads"),
            P("batch", None),
            P("heads", "batch"),
        ),
        out_specs=P("heads", "seq", "batch"),
        check_vma=False,
    )
```

```python
import functools

import jax
import jax.numpy as jnp
from jax import lax
from jax.experimental import pallas as pl
from jax.experimental.pallas import tpu as pltpu
from jax.sharding import PartitionSpec as P

MESH = pl.DeviceIdType.MESH
HEAD = 128
DOCS = 16
LAG = 3
DIRECT = 2
EARLY = ((0, 64), (64, 64))
CHUNKS = tuple((32 * c, 32) for c in range(8))
LOWEST = -1e30
SCALE = (HEAD ** -0.5) * 1.4426950408889634


def kernel(
    q_hbm, k_hbm, v_hbm, docs, w_hbm, outv,
    qv, qt, kv, vt, bias, top, total, shrink, raw, soft, acc, gathered, weight, partial, near, final,
    load_sem, kv_recv, next_send, side_send, far_send, wrap_send, ag_send, ag_recv, rs_send, rs_recv,
):
    s = lax.axis_index("seq")
    x = lax.axis_index("heads")
    y = lax.axis_index("batch")
    seqs, xs, ys = lax.axis_size("seq"), lax.axis_size("heads"), lax.axis_size("batch")
    z = s // 2
    odd = s % 2
    rows = qv.shape[0]
    heads = acc.shape[0] // 2
    half = rows // 2
    right, left, across = (x + 1) % xs, (x + xs - 1) % xs, (x + 2) % xs
    up, down, opposite = (y + 1) % ys, (y + ys - 1) % ys, (y + 2) % ys

    def remote(src, dst, send, recv, **where):
        return pltpu.make_async_remote_copy(
            src_ref=src, dst_ref=dst, send_sem=send, recv_sem=recv, device_id=where, device_id_type=MESH
        )

    def load(g, i):
        src = (k_hbm, v_hbm)[i]
        return pltpu.make_async_copy(
            src.at[0, :, g * HEAD : (g + 1) * HEAD], kv.at[0, g, i], load_sem.at[2 * g + i]
        )

    load_q = pltpu.make_async_copy(q_hbm.at[0], qv, load_sem.at[4])
    load_w = pltpu.make_async_copy(w_hbm, weight, load_sem.at[5])
    for g in range(2):
        for i in range(2):
            load(g, i).start()
    load_q.start()

    barrier = pltpu.get_barrier_semaphore()
    for by in (1, 2, 6, 7, 9, 10, seqs - 2, seqs - 1):
        pl.semaphore_signal(barrier, inc=1, device_id={"seq": (s + by) % seqs}, device_id_type=MESH)
    for peer in (right, left):
        pl.semaphore_signal(barrier, inc=1, device_id={"heads": peer}, device_id_type=MESH)
    for peer in (up, down, opposite):
        pl.semaphore_signal(barrier, inc=1, device_id={"batch": peer}, device_id_type=MESH)
    pl.semaphore_wait(barrier, 13)

    def to_next(t, g, i):
        slot = jnp.minimum(2 * t + 2, 8)
        return remote(
            kv.at[2 * t, g, i], kv.at[slot, g, i], next_send.at[jnp.minimum(t, 3), g, i], kv_recv.at[slot, g, i],
            seq=jnp.minimum(s + 2, seqs - 1),
        )

    def to_side(t, g, i):
        slot = jnp.maximum(2 * t + 1 - 2 * odd, 0)
        return remote(
            kv.at[2 * t, g, i], kv.at[slot, g, i], side_send.at[t, g, i], kv_recv.at[slot, g, i],
            seq=s + 1 - 2 * odd,
        )

    def to_far(g, i):
        return remote(
            kv.at[8, g, i, half:], kv.at[9, g, i, half:], far_send.at[g, i], kv_recv.at[9, g, i],
            seq=jnp.minimum(s + 1, seqs - 1),
        )

    def to_jump(i):
        return remote(
            kv.at[0, 0, i, half:], kv.at[9, 0, i, half:], far_send.at[2, i], kv_recv.at[9, 0, i], seq=(s + 9) % seqs
        )

    def to_wrap(i):
        return remote(kv.at[0, 1, i], kv.at[10, 1, i], wrap_send.at[0, i], kv_recv.at[10, 1, i], seq=(s + 10) % seqs)

    def to_back(i):
        return remote(
            kv.at[10, 1, i], kv.at[8, 1, i], wrap_send.at[1, i], kv_recv.at[8, 1, i], seq=(s + seqs - 2) % seqs
        )

    def to_corner(i):
        return remote(
            kv.at[10, 1, i, half:], kv.at[9, 1, i, half:], wrap_send.at[2, i], kv_recv.at[9, 1, i],
            seq=jnp.maximum(s - 1, 0),
        )

    def sends_next(t, g):
        return (z >= t) & (t <= 3 - g) & (s + 2 < seqs)

    def sends_side(t):
        return (z >= t) & (t >= odd) & (t <= 3 + odd)

    sends_far = (z >= 4) & (odd == 0)
    sends_jump = (s < 6) & (odd == 1)

    sends_wrap = s < 8
    transit = (s >= 10) | (s < 2)
    corner = (s >= 10) & (odd == 1)

    def forward(t, g, i):
        @pl.when(sends_next(t, g))
        def _():
            to_next(t, g, i).start()

        @pl.when(sends_side(t))
        def _():
            to_side(t, g, i).start()

        @pl.when(sends_far & (t == 4))
        def _():
            to_far(g, i).start()

    def arrived(slot, g, i):
        remote(kv.at[slot, g, i], kv.at[slot, g, i], next_send.at[0, 0, 0], kv_recv.at[slot, g, i], seq=s).wait_recv()

    for g in range(2):
        for i in range(2):
            load(g, i).wait()
            forward(0, g, i)

    for i in range(2):
        @pl.when(sends_wrap)
        def _():
            to_wrap(i).start()

        @pl.when(sends_jump)
        def _():
            to_jump(i).start()

    q_pos = s * rows + lax.broadcasted_iota(jnp.int32, (1, rows), 1)
    starts = jnp.zeros((1, rows), jnp.int32)
    ended = jnp.int32(0)
    for d in range(DOCS):
        length = docs[0, d]
        ended = ended + length
        starts = starts + jnp.where(q_pos >= ended, length, 0)

    @pl.loop(0, 10)
    def _(slot):
        k_pos = (s - slot) * rows + lax.broadcasted_iota(jnp.int32, (rows, rows), 0)
        q_all = s * rows + lax.broadcasted_iota(jnp.int32, (rows, rows), 1)
        bias[slot] = jnp.where((k_pos >= starts) & (k_pos <= q_all), 0.0, LOWEST)

    vt[HEAD:] = jnp.ones((vt.shape[0] - HEAD, rows), jnp.bfloat16)
    load_q.wait()
    load_w.start()

    @pl.loop(0, 2 * heads)
    def _(h):
        qt[h] = qv[:, pl.ds(pl.multiple_of(h * HEAD, HEAD), HEAD)].T

    def attend(slot, g, low, columns):
        count = rows - low
        keys = kv.at[slot, g, 0]
        mine = pl.ds(g * heads, heads)
        queries, high, sums_of, mixed = qt.at[mine], top.at[mine], total.at[mine], acc.at[mine]
        shift = bias.at[slot]
        vt[:HEAD, :count] = kv[slot, g, 1, low:].T

        def score(h):
            scores = jnp.dot(keys[low:], queries[h, :, :columns], preferred_element_type=jnp.float32)
            scores = scores + shift[low:, :columns]
            raw[h, :count, :columns] = scores
            before = high[h, :, :columns]
            now = jnp.maximum(before, jnp.max(scores, axis=0, keepdims=True))
            shrink[h, :, :columns] = jnp.exp2((before - now) * SCALE)
            high[h, :, :columns] = now

        def weigh(h):
            weights = jnp.exp2((raw[h, :count, :columns] - high[h, :, :columns]) * SCALE)
            soft[h, :count, :columns] = weights.astype(jnp.bfloat16)

        def mix(h):
            summed = jnp.dot(vt[:, :count], soft[h, :count, :columns], preferred_element_type=jnp.float32)
            mixed[h, :, :columns] = mixed[h, :, :columns] * shrink[h, :, :columns] + summed[:HEAD]
            sums_of[h, :, :columns] = sums_of[h, :, :columns] * shrink[h, :, :columns] + summed[HEAD : HEAD + 1]

        for i in range(heads + 2 * LAG):
            if i < heads:
                score(i)
            if 0 <= i - LAG < heads:
                weigh(i - LAG)
            if 0 <= i - 2 * LAG < heads:
                mix(i - 2 * LAG)

    middle = gathered.shape[3] // 2
    early = sum(n for _, n in EARLY)
    items = [(slice(1, 2), o, n) for o, n in EARLY]
    items += [(slice(0, 1) if o < early else slice(0, 2), o, n) for o, n in CHUNKS]

    def copies_of(k, holder, far):
        groups, o, n = items[k]
        a = gathered.at[groups, holder[0], o : o + n]
        b = gathered.at[groups, holder[1], o : o + n]
        if far and k == DIRECT:
            return (remote(a, a, ag_send.at[k, 2], ag_recv.at[k, 2], batch=opposite),)
        if far:
            a, b = a.at[:, :, :middle], b.at[:, :, middle:]
        return (
            remote(a, a, ag_send.at[k, 2 * far], ag_recv.at[k, 2 * far], batch=up),
            remote(b, b, ag_send.at[k, 2 * far + 1], ag_recv.at[k, 2 * far + 1], batch=down),
        )

    def onward(k):
        return copies_of(k, (y, y) if k == DIRECT else (down, up), 1)

    def start_own(k):
        for copy in (*onward(k), *copies_of(k, (y, y), 0)) if k == DIRECT else copies_of(k, (y, y), 0):
            copy.start()

    def relay(k):
        for i, arriving in enumerate(copies_of(k, (down, up), 0)):
            arriving.wait_recv()
            if k != DIRECT:
                onward(k)[i].start()

    def settle(k):
        for arriving in copies_of(k, (opposite, opposite), 1):
            arriving.wait_recv()

    def normalize(g, low):
        mine = pl.ds(g * heads, heads)
        for h in range(heads):
            done = acc.at[mine][h, :, low : low + half] * (1.0 / total.at[mine][h, :, low : low + half])
            gathered[g, y, low : low + half, h * HEAD : (h + 1) * HEAD] = done.T.astype(jnp.bfloat16)

    top[...] = jnp.full(top.shape, LOWEST, jnp.float32)
    total[...] = jnp.zeros(total.shape, jnp.float32)

    @pl.loop(0, 2 * heads)
    def _(h):
        acc[h] = jnp.zeros(acc.shape[1:], jnp.float32)

    @pl.loop(0, 14)
    def _(m):
        n, g = m // 2, m % 2
        t = (n + 1) // 2
        lane = n % 2 == 0
        here = (z >= t) & (n >= 1) & (n <= 8)
        side = n - 2 * (1 - odd)

        @pl.when(here)
        def _():
            arrived(2 * t, 1 - n % 2, g)
            forward(t, 1 - n % 2, g)

        slot = jnp.where(lane, n, jnp.maximum(side, 0))
        taken = jnp.where(lane, (n <= 8) & (z >= t), (side >= 1) & (side <= 7) & (s >= side))

        @pl.when(taken)
        def _():
            @pl.when(n % 2 == 1)
            def _():
                for i in range(2):
                    arrived(slot, g, i)

            attend(slot, g, 0, rows)

        @pl.when((m == 9) & transit)
        def _():
            for i in range(2):
                arrived(10, 1, i)
                to_back(i).start()

                @pl.when(corner)
                def _():
                    to_corner(i).start()

    @pl.loop(0, 2)
    def _(r):
        g = 1 - r

        @pl.loop(0, 5)
        def _(q):
            lane = q == 2
            n = jnp.where(q == 0, 7, jnp.where(lane, 8, 9))
            side = n - 2 * (1 - odd)

            @pl.when(lane & (z >= 4))
            def _():
                for i in range(2):
                    arrived(8, g, i)
                    forward(4, g, i)

            slot = jnp.where(lane, 8, side)

            @pl.when((q % 4 != 1) & (q < 4) & jnp.where(lane, z >= 4, (side <= 7) & (s >= side)))
            def _():
                @pl.when(q != 2)
                def _():
                    for i in range(2):
                        arrived(jnp.minimum(slot, 9), g, i)

                attend(jnp.minimum(slot, 8), g, 0, rows)

            @pl.when((q == 1 + 3 * odd) & (s >= 9))
            def _():
                for i in range(2):
                    remote(
                        kv.at[9, g, i, half:], kv.at[9, g, i, half:], far_send.at[0, i], kv_recv.at[9, g, i], seq=s
                    ).wait_recv()
                attend(9, g, half, half)

        normalize(g, 0)

        @pl.when(r == 0)
        def _():
            start_own(0)

        @pl.when(r == 1)
        def _():
            start_own(2)

        normalize(g, half)

        @pl.when(r == 0)
        def _():
            start_own(1)

    part = weight.shape[1] // 2
    wide = 512

    def sums(c):
        o, n = CHUNKS[c]
        some = slice(o, o + n)
        table = (
            (partial.at[across, some, :part], near.at[0, some], right),
            (partial.at[across, some, part:], near.at[1, some], left),
            (partial.at[right, some, part:], final.at[0, some, part:], right),
            (partial.at[left, some, :part], final.at[1, some, :part], left),
            (partial.at[right, some, :part], final.at[0, some, :part], right),
            (partial.at[left, some, part:], final.at[1, some, part:], left),
        )
        return [
            functools.partial(remote, src, dst, rs_send.at[c, i], rs_recv.at[c, i], heads=to)
            for i, (src, dst, to) in enumerate(table)
        ]

    def project(c):
        o, n = CHUNKS[c]
        for k, (e, many) in enumerate(EARLY):
            if o == e:
                settle(k)
        settle(len(EARLY) + c)
        lhs = jnp.concatenate([gathered[g, :, o : o + n].reshape(ys * n, -1) for g in range(2)], axis=1)

        for side in range(2):
            @pl.loop(side * part // wide, (side + 1) * part // wide)
            def _(m):
                columns = pl.ds(pl.multiple_of(m * wide, wide), wide)
                product = jnp.dot(lhs, weight[:, columns], preferred_element_type=jnp.float32)
                partial[:, o : o + n, columns] = product.astype(jnp.bfloat16).reshape(ys, n, wide)

            for i in ((0, 3), (1, 2))[side]:
                sums(c)[i]().start()

    def send_second(c):
        o, n = CHUNKS[c]
        copies = sums(c)
        for i, to, low in ((0, right, 0), (1, left, part)):
            copies[i]().wait_recv()
            partial[to, o : o + n, low : low + part] = (
                partial[to, o : o + n, low : low + part].astype(jnp.float32)
                + near[i, o : o + n].astype(jnp.float32)
            ).astype(jnp.bfloat16)
            copies[4 + i]().start()

    def finish(c):
        o, n = CHUNKS[c]
        copies = sums(c)
        for i in range(2, 6):
            copies[i]().wait_recv()
        value = (
            partial[x, o : o + n].astype(jnp.float32)
            + final[0, o : o + n].astype(jnp.float32)
            + final[1, o : o + n].astype(jnp.float32)
        )
        outv[0, o : o + n] = value.astype(jnp.bfloat16)

    load_w.wait()
    chunks = len(CHUNKS)
    first_chunk = len(EARLY)
    relay(0)
    start_own(first_chunk + 1)
    relay(1)
    for i in range(chunks + 3):
        if i == 1:
            project(0)
        if i < chunks:
            relay(first_chunk + i)
        if i + 2 < chunks:
            start_own(first_chunk + i + 2)
        if 1 <= i - 1 < chunks:
            project(i - 1)
        if 0 <= i - 2 < chunks:
            send_second(i - 2)
        if i >= 3:
            finish(i - 3)

    @pl.loop(0, 5)
    def _(t):
        for g in range(2):
            for i in range(2):
                @pl.when(sends_next(t, g))
                def _():
                    to_next(t, g, i).wait_send()

                @pl.when(sends_side(t))
                def _():
                    to_side(t, g, i).wait_send()

    for i in range(2):
        for g in range(2):
            @pl.when(sends_far)
            def _():
                to_far(g, i).wait_send()

        @pl.when(sends_jump)
        def _():
            to_jump(i).wait_send()

        @pl.when(sends_wrap)
        def _():
            to_wrap(i).wait_send()

        @pl.when(transit)
        def _():
            to_back(i).wait_send()

        @pl.when(corner)
        def _():
            to_corner(i).wait_send()

    for k in range(len(items)):
        for copy in (*copies_of(k, (y, y), 0), *onward(k)):
            copy.wait_send()
    for c in range(chunks):
        for copy in sums(c):
            copy().wait_send()


def per_device(queries, keys, values, doc_lengths, out_weight):
    rows, q_width = queries.shape[1:]
    kv_heads = keys.shape[2] // HEAD
    depth, columns = out_weight.shape
    ys = lax.axis_size("batch")
    heads = q_width // HEAD // kv_heads
    items = len(EARLY) + len(CHUNKS)
    bf16, f32 = jnp.bfloat16, jnp.float32
    anywhere = pl.BlockSpec(memory_space=pl.ANY)
    dma = pltpu.SemaphoreType.DMA
    held = pl.pallas_call(
        kernel,
        out_shape=pltpu.VMEM((1, rows, columns), bf16),
        in_specs=[anywhere, anywhere, anywhere, pl.BlockSpec(memory_space=pltpu.SMEM), anywhere],
        out_specs=pl.BlockSpec(memory_space=pltpu.VMEM),
        scratch_shapes=[
            pltpu.VMEM((rows, q_width), bf16),
            pltpu.VMEM((kv_heads * heads, HEAD, rows), bf16),
            pltpu.VMEM((11, kv_heads, 2, rows, HEAD), bf16),
            pltpu.VMEM((HEAD + 16, rows), bf16),
            pltpu.VMEM((10, rows, rows), f32),
            pltpu.VMEM((kv_heads * heads, 1, rows), f32),
            pltpu.VMEM((kv_heads * heads, 1, rows), f32),
            pltpu.VMEM((heads, 1, rows), f32),
            pltpu.VMEM((heads, rows, rows), f32),
            pltpu.VMEM((heads, rows, rows), bf16),
            pltpu.VMEM((kv_heads * heads, HEAD, rows), f32),
            pltpu.VMEM((kv_heads, ys, rows, heads * HEAD), bf16),
            pltpu.VMEM((depth, columns), bf16),
            pltpu.VMEM((ys, rows, columns), bf16),
            pltpu.VMEM((2, rows, columns // 2), bf16),
            pltpu.VMEM((2, rows, columns), bf16),
            dma((6,)),
            dma((11, 2, 2)),
            dma((4, 2, 2)),
            dma((5, 2, 2)),
            dma((3, 2)),
            dma((3, 2)),
            dma((items, 4)),
            dma((items, 4)),
            dma((len(CHUNKS), 6)),
            dma((len(CHUNKS), 6)),
        ],
        compiler_params=pltpu.CompilerParams(
            collective_id=0, has_side_effects=True, vmem_limit_bytes=60 * 1024 * 1024
        ),
    )(queries, keys, values, doc_lengths, out_weight)
    return held


def solution(mesh):
    return jax.shard_map(
        per_device,
        mesh=mesh,
        in_specs=(
            P("batch", "seq", "heads"),
            P("batch", "seq", "heads"),
            P("batch", "seq", "heads"),
            P("batch", None),
            P("heads", "batch"),
        ),
        out_specs=P("heads", "seq", "batch"),
        check_vma=False,
    )
```
